32 devices in a mesh: gz: 8 (over z, y), pa: 4 (over x, core).
Axes of the slice: x: 2, y: 2, z: 4, core: 2. Of those that a mesh axis runs over, the one named last changes fastest.
Arguments:
- density: bfloat16 [64, 1024, 1024], P('gz', 'pa'), may hold values from -6 to 6
- green: float32 [128, 1024, 1024], P('gz', 'pa'), may hold values from 0.1 to 3
Outputs:
- potential: float32 [64, 1024, 1024], P('gz', 'pa')
The draws below stay inside these ranges and needn't reach their ends.
All inputs are finite; a program needn't handle non-finite values.
Results may differ from the reference program's by a relative error of at most 0.02.
Values may be sent and summed in bfloat16 or wider, within the bound.
A program may use at most 192 MiB of HBM per device.

```python
import math
import jax
import jax.numpy as jnp
from jax import lax

NX = 1024
NY = 1024
NZ = 64
M = 128
N_GZ = 8


def level_of(key, dims, cuts, least, high):
    level = 1.0
    for axis_at, shards_of in cuts:
        steps = jax.random.uniform(jax.random.fold_in(jax.random.fold_in(key, 6), axis_at), (shards_of,), jnp.float32, least / len(cuts), high / len(cuts))
        level = level * jnp.repeat(jnp.exp(steps), dims[axis_at] // shards_of).reshape((-1,) + (1,) * (len(dims) - 1 - axis_at))
    return level


def scatter_about(stream_key, extent, deviation, limit, cuts=(), kind=jnp.bfloat16):
    drawn = jax.random.normal(stream_key, extent, jnp.float32) * deviation
    if len(cuts) > 0:
        drawn = level_of(stream_key, extent, cuts, -0.22, 0.18) * drawn
    return jnp.clip(drawn, min=-limit, max=limit).astype(kind)


def setup_inputs(seed: int = 0) -> dict:
    arg_keys = jax.random.split(jax.random.key(seed), 3)
    return {
        "density": scatter_about(arg_keys[0], (NZ, NX, NY), 1.0, 6.0, ((0, 8), (1, 4))),
        "green": jnp.clip(jnp.exp(math.log(3.0) - 3.4011974 * jax.random.uniform(arg_keys[1], (M, NY, NX), jnp.float32) ** level_of(arg_keys[1], (M, NY, NX), ((0, 8), (1, 4)), -0.2, 0.2)), 0.1, 3.0),
    }


def cas_table(rows, cols, length):
    product = (rows[:, None] * cols[None, :]) % length
    angle = product.astype(jnp.float32) * (2.0 * math.pi / length)
    return (jnp.cos(angle) + jnp.sin(angle)).astype(jnp.bfloat16)


def blocked_sum(tables, pieces, rows, columns):
    def add_block(total, pair):
        table, piece = pair
        term = jnp.dot(table, piece, precision=lax.Precision.HIGHEST, preferred_element_type=jnp.float32).astype(jnp.bfloat16)
        term = lax.optimization_barrier(term)
        return total + term.astype(jnp.float32), None

    total, _ = lax.scan(add_block, jnp.zeros((rows, columns), jnp.float32), (tables, pieces))
    return total


def reference(density, green):
    z_cells, x_cells, y_cells = density.shape
    z_freqs = 2 * z_cells
    z_slab = z_cells // N_GZ
    k_block = z_freqs // N_GZ
    columns = x_cells * y_cells
    highest = lax.Precision.HIGHEST
    f_index = jnp.arange(z_freqs, dtype=jnp.int32)
    z_index = jnp.arange(z_cells, dtype=jnp.int32)
    forward_tables = cas_table(f_index, z_index, z_freqs).astype(jnp.float32).reshape(z_freqs, N_GZ, z_slab).transpose(1, 0, 2)
    slabs = density.astype(jnp.float32).reshape(N_GZ, z_slab, columns)
    zspec = blocked_sum(forward_tables, slabs, z_freqs, columns).astype(jnp.bfloat16).reshape(z_freqs, x_cells, y_cells)
    cas_y = cas_table(jnp.arange(y_cells, dtype=jnp.int32), jnp.arange(y_cells, dtype=jnp.int32), y_cells).astype(jnp.float32)
    cas_x = cas_table(jnp.arange(x_cells, dtype=jnp.int32), jnp.arange(x_cells, dtype=jnp.int32), x_cells).astype(jnp.float32)
    yspec = jnp.einsum('kxy,vy->kxv', zspec.astype(jnp.float32), cas_y, precision=highest).astype(jnp.bfloat16)
    xspec = jnp.einsum('kxv,ux->kvu', yspec.astype(jnp.float32), cas_x, precision=highest)
    weighted = (green * xspec).astype(jnp.bfloat16)
    yback = jnp.einsum('kvu,xu->kxv', weighted.astype(jnp.float32), cas_x, precision=highest).astype(jnp.bfloat16)
    zback = jnp.einsum('kxv,yv->kxy', yback.astype(jnp.float32), cas_y, precision=highest).astype(jnp.bfloat16)
    back_tables = cas_table(z_index, f_index, z_freqs).astype(jnp.float32).reshape(z_cells, N_GZ, k_block).transpose(1, 0, 2)
    blocks = zback.astype(jnp.float32).reshape(N_GZ, k_block, columns)
    total = blocked_sum(back_tables, blocks, z_cells, columns)
    scale = 1.0 / (x_cells * y_cells * z_freqs)
    return (total * scale).reshape(z_cells, x_cells, y_cells)
```

```python
import math

import jax
import jax.numpy as jnp
from jax import lax
from jax.experimental import pallas as pl
from jax.experimental.pallas import tpu as pltpu
from jax.sharding import PartitionSpec as P

BF = jnp.bfloat16
F32 = jnp.float32


def cas_table(rows, cols, length):
    product = rows[:, None] * cols[None, :] % length
    angle = product.astype(F32) * (2.0 * math.pi / length)
    return (jnp.cos(angle) + jnp.sin(angle)).astype(BF)


def square_table(n):
    index = jnp.arange(n, dtype=jnp.int32)
    return cas_table(index, index, n)


def cost(flops, *arrays):
    size = sum(math.prod(a.shape) * a.dtype.itemsize for a in arrays)
    return pl.CostEstimate(flops=flops, bytes_accessed=size, transcendentals=0)


def dot(a, b):
    return jnp.dot(a, b, preferred_element_type=F32)


def dot_t(a, b):
    return lax.dot_general(a, b, (((1,), (1,)), ((), ())), preferred_element_type=F32)


def green_split(green, groups):
    k, v, u = green.shape
    share = v // groups

    def body(g_ref, o_ref):
        for j in range(groups):
            o_ref[j, 0] = g_ref[0, j * share : (j + 1) * share, :].astype(BF)

    out = jax.ShapeDtypeStruct((groups, k, share, u), BF)
    return pl.pallas_call(
        body,
        grid=(k,),
        in_specs=[pl.BlockSpec((1, v, u), lambda i: (i, 0, 0))],
        out_specs=pl.BlockSpec((groups, 1, share, u), lambda i: (0, i, 0, 0)),
        out_shape=out,
        cost_estimate=cost(0, green, out),
        name="green_split",
    )(green)


def y_forward(density, table, pencils):
    z, x, y = density.shape
    block = y // pencils

    def body(d_ref, t_ref, o_ref):
        for p in range(pencils):
            rows = t_ref[p * block : (p + 1) * block, :]
            o_ref[p, 0] = dot_t(rows, d_ref[0]).astype(BF)

    out = jax.ShapeDtypeStruct((pencils, z, block, x), BF)
    return pl.pallas_call(
        body,
        grid=(z,),
        in_specs=[
            pl.BlockSpec((1, x, y), lambda i: (i, 0, 0)),
            pl.BlockSpec((y, y), lambda i: (0, 0)),
        ],
        out_specs=pl.BlockSpec((pencils, 1, block, x), lambda i: (0, i, 0, 0)),
        out_shape=out,
        cost_estimate=cost(2 * z * x * y * y, density, table, out),
        name="y_forward",
    )(density, table)


def x_forward(moved, table, groups):
    pencils, z, v, x = moved.shape
    u = pencils * x
    share = v // groups

    def body(m_ref, t_ref, o_ref):
        total = dot(m_ref[0, 0], t_ref[0:x, :])
        for p in range(1, pencils):
            total += dot(m_ref[p, 0], t_ref[p * x : (p + 1) * x, :])
        total = total.astype(BF)
        for j in range(groups):
            o_ref[j, 0] = total[j * share : (j + 1) * share, :]

    out = jax.ShapeDtypeStruct((groups, z, share, u), BF)
    return pl.pallas_call(
        body,
        grid=(z,),
        in_specs=[
            pl.BlockSpec((pencils, 1, v, x), lambda i: (0, i, 0, 0)),
            pl.BlockSpec((u, u), lambda i: (0, 0)),
        ],
        out_specs=pl.BlockSpec((groups, 1, share, u), lambda i: (0, i, 0, 0)),
        out_shape=out,
        cost_estimate=cost(2 * z * v * u * u, moved, table, out),
        name="x_forward",
    )(moved, table)


def z_weight(planes, green, table):
    z, v, u = planes.shape
    k = green.shape[0]
    if v % 8:
        spec = jnp.einsum("kz,zvu->kvu", table, planes, preferred_element_type=F32)
        weighted = (green.astype(F32) * spec).astype(BF)
        return jnp.einsum("kz,kvu->zvu", table, weighted, preferred_element_type=F32).astype(BF)
    lanes = min(u, 512)
    rows = 16 if v % 16 == 0 else 8
    eye = jnp.eye(8, dtype=BF)
    wide = jnp.einsum("kz,ab->kazb", table, eye).reshape(k * 8, z * 8)
    tall = wide.T

    def body(s_ref, g_ref, w_ref, t_ref, o_ref):
        for i in range(0, rows, 8):
            flat = s_ref[:, i : i + 8, :].astype(F32).reshape(z * 8, lanes).astype(BF)
            spec = dot(w_ref[...], flat)
            weight = g_ref[:, i : i + 8, :].astype(F32).reshape(k * 8, lanes)
            back = dot(t_ref[...], (spec * weight).astype(BF))
            o_ref[:, i : i + 8, :] = back.reshape(z, 8, lanes).astype(BF)

    out = jax.ShapeDtypeStruct((z, v, u), BF)
    at = lambda i, j: (0, i, j)
    whole = lambda i, j: (0, 0)
    return pl.pallas_call(
        body,
        grid=(v // rows, u // lanes),
        in_specs=[
            pl.BlockSpec((z, rows, lanes), at),
            pl.BlockSpec((k, rows, lanes), at),
            pl.BlockSpec((k * 8, z * 8), whole),
            pl.BlockSpec((z * 8, k * 8), whole),
        ],
        out_specs=pl.BlockSpec((z, rows, lanes), at),
        out_shape=out,
        compiler_params=pltpu.CompilerParams(vmem_limit_bytes=60 * 2**20),
        cost_estimate=cost(32 * z * k * v * u, planes, green, out),
        name="z_weight",
    )(planes, green, wide, tall)


def x_inverse(back, table, pencils):
    groups, z, share, u = back.shape
    v = groups * share
    x = u // pencils

    def body(b_ref, t_ref, o_ref):
        rows = jnp.concatenate([b_ref[j, 0] for j in range(groups)], axis=0)
        for p in range(pencils):
            o_ref[p, 0] = dot_t(t_ref[p * x : (p + 1) * x, :], rows).astype(BF)

    out = jax.ShapeDtypeStruct((pencils, z, x, v), BF)
    return pl.pallas_call(
        body,
        grid=(z,),
        in_specs=[
            pl.BlockSpec((groups, 1, share, u), lambda i: (0, i, 0, 0)),
            pl.BlockSpec((u, u), lambda i: (0, 0)),
        ],
        out_specs=pl.BlockSpec((pencils, 1, x, v), lambda i: (0, i, 0, 0)),
        out_shape=out,
        cost_estimate=cost(2 * z * v * u * u, back, table, out),
        name="x_inverse",
    )(back, table)


def y_inverse(returned, table, scale):
    pencils, z, x, v = returned.shape
    y = pencils * v

    def body(r_ref, t_ref, o_ref):
        total = dot(r_ref[0, 0], t_ref[0:v, :])
        for p in range(1, pencils):
            total += dot(r_ref[p, 0], t_ref[p * v : (p + 1) * v, :])
        o_ref[0] = total * scale

    out = jax.ShapeDtypeStruct((z, x, y), F32)
    return pl.pallas_call(
        body,
        grid=(z,),
        in_specs=[
            pl.BlockSpec((pencils, 1, x, v), lambda i: (0, i, 0, 0)),
            pl.BlockSpec((y, y), lambda i: (0, 0)),
        ],
        out_specs=pl.BlockSpec((1, x, y), lambda i: (i, 0, 0)),
        out_shape=out,
        cost_estimate=cost(2 * z * x * y * y, returned, table, out),
        name="y_inverse",
    )(returned, table)


def exchange(a, axis):
    return lax.all_to_all(a, axis, split_axis=0, concat_axis=0, tiled=True)


def local(density, green):
    z_slab, x_local, y_cells = density.shape
    k_block, y_local, x_cells = green.shape
    groups = lax.axis_size("gz")
    pencils = lax.axis_size("pa")
    z_cells = z_slab * groups
    z_freqs = k_block * groups
    share = y_local // groups
    weights = exchange(green_split(green, groups), "gz").reshape(z_freqs, share, x_cells)
    cas_y = square_table(y_cells)
    cas_x = cas_y if x_cells == y_cells else square_table(x_cells)
    cas_m = cas_table(
        jnp.arange(z_freqs, dtype=jnp.int32), jnp.arange(z_cells, dtype=jnp.int32), z_freqs
    )
    moved = exchange(y_forward(density, cas_y, pencils), "pa")
    planes = exchange(x_forward(moved, cas_x, groups), "gz").reshape(z_cells, share, x_cells)
    back = z_weight(planes, weights, cas_m).reshape(groups, z_slab, share, x_cells)
    back = exchange(back, "gz")
    returned = exchange(x_inverse(back, cas_x, pencils), "pa")
    return y_inverse(returned, cas_y, 1.0 / (x_cells * y_cells * z_freqs))


def solution(mesh):
    return jax.shard_map(
        local,
        mesh=mesh,
        in_specs=(P("gz", "pa", None), P("gz", "pa", None)),
        out_specs=P("gz", "pa", None),
        check_vma=False,
    )
```

```python
import math

import jax
import jax.numpy as jnp
from jax import lax
from jax.experimental import pallas as pl
from jax.experimental.pallas import tpu as pltpu
from jax.sharding import PartitionSpec as P


BF = jnp.bfloat16
F32 = jnp.float32
CHUNKS = 2


def cas_table(rows, cols, length):
    product = rows[:, None] * cols[None, :] % length
    angle = product.astype(F32) * (2.0 * math.pi / length)
    return (jnp.cos(angle) + jnp.sin(angle)).astype(BF)


def square_table(n):
    index = jnp.arange(n, dtype=jnp.int32)
    return cas_table(index, index, n)


def cost(flops, *arrays):
    size = sum(math.prod(a.shape) * a.dtype.itemsize for a in arrays)
    return pl.CostEstimate(flops=flops, bytes_accessed=size, transcendentals=0)


def dot(a, b):
    return jnp.dot(a, b, preferred_element_type=F32)


def dot_t(a, b):
    return lax.dot_general(a, b, (((1,), (1,)), ((), ())), preferred_element_type=F32)


def on_rank(body, grid, in_specs, out_specs, out_shape, cost_estimate, **more):
    spec = pltpu.PrefetchScalarGridSpec(
        num_scalar_prefetch=1, grid=grid, in_specs=in_specs, out_specs=out_specs
    )
    return pl.pallas_call(
        lambda r, *refs: body(*refs),
        grid_spec=spec,
        out_shape=out_shape,
        cost_estimate=cost_estimate,
        **more,
    )


def green_piece(green, rank, step, groups):
    k, v, u = green.shape
    share = v // groups
    cut = math.gcd(k, 4)
    pieces = green.reshape(k, groups, share, u)

    def body(g_ref, o_ref):
        o_ref[...] = g_ref[:, 0].astype(BF)

    out = jax.ShapeDtypeStruct((k, share, u), BF)
    return on_rank(
        body,
        (k // cut,),
        [pl.BlockSpec((cut, 1, share, u), lambda i, r: (i, lax.rem(r[0] + step, groups), 0, 0))],
        pl.BlockSpec((cut, share, u), lambda i, r: (i, 0, 0)),
        out,
        cost(0, out, out, out),
    )(rank, pieces)


def shift(a, axis, step):
    n = lax.axis_size(axis)
    return lax.ppermute(a, axis, [(i, (i + step) % n) for i in range(n)])


def y_forward(density, table, pencils):
    z, x, y = density.shape
    block = y // pencils

    def body(d_ref, t_ref, o_ref):
        for p in range(pencils):
            rows = t_ref[p * block : (p + 1) * block, :]
            o_ref[p, 0] = dot_t(rows, d_ref[0]).astype(BF)

    out = jax.ShapeDtypeStruct((pencils, z, block, x), BF)
    return pl.pallas_call(
        body,
        grid=(z,),
        in_specs=[
            pl.BlockSpec((1, x, y), lambda i: (i, 0, 0)),
            pl.BlockSpec((y, y), lambda i: (0, 0)),
        ],
        out_specs=pl.BlockSpec((pencils, 1, block, x), lambda i: (0, i, 0, 0)),
        out_shape=out,
        cost_estimate=cost(2 * z * x * y * y, density, table, out),
        name="y_forward",
    )(density, table)


def x_forward(moved, table, groups):
    pencils, z, v, x = moved.shape
    u = pencils * x
    share = v // groups

    def body(m_ref, t_ref, o_ref):
        total = dot(m_ref[0, 0], t_ref[0:x, :])
        for p in range(1, pencils):
            total += dot(m_ref[p, 0], t_ref[p * x : (p + 1) * x, :])
        total = total.astype(BF)
        for j in range(groups):
            o_ref[j, 0] = total[j * share : (j + 1) * share, :]

    out = jax.ShapeDtypeStruct((groups, z, share, u), BF)
    return pl.pallas_call(
        body,
        grid=(z,),
        in_specs=[
            pl.BlockSpec((pencils, 1, v, x), lambda i: (0, i, 0, 0)),
            pl.BlockSpec((u, u), lambda i: (0, 0)),
        ],
        out_specs=pl.BlockSpec((groups, 1, share, u), lambda i: (0, i, 0, 0)),
        out_shape=out,
        cost_estimate=cost(2 * z * v * u * u, moved, table, out),
        name="x_forward",
    )(moved, table)


def z_weight(planes, greens, table, chunks):
    z, v, u = planes.shape
    groups = len(greens)
    part = greens[0].shape[0]
    k = part * groups
    depth = z // groups // chunks
    if v % 8:
        green = jnp.concatenate(greens, axis=0)
        spec = jnp.einsum("kz,zvu->kvu", table, planes, preferred_element_type=F32)
        weighted = (green.astype(F32) * spec).astype(BF)
        back = jnp.einsum("kz,kvu->zvu", table, weighted, preferred_element_type=F32).astype(BF)
        back = back.reshape(groups, chunks, depth, v, u)
        return [back[:, c] for c in range(chunks)]
    lanes = min(u, 512)
    rows = 16 if v % 16 == 0 else 8
    row = jnp.arange(8, dtype=jnp.int32)

    def widen(t):
        same = (jnp.arange(8 * t.shape[0]) % 8)[:, None] == (jnp.arange(8 * t.shape[1]) % 8)[None]
        return jnp.where(same, jnp.repeat(jnp.repeat(t, 8, axis=0), 8, axis=1), 0).astype(BF)

    wide = widen(table)
    tall = widen(table.T)

    def body(s_ref, *refs):
        g_refs, (w_ref, t_ref), o_refs = refs[:groups], refs[groups : groups + 2], refs[groups + 2 :]
        for i in range(0, rows, 8):
            flat = s_ref[:, i : i + 8, :].astype(F32).reshape(z * 8, lanes).astype(BF)
            spec = dot(w_ref[...], flat)
            weight = jnp.concatenate(
                [g[:, i : i + 8, :].astype(F32).reshape(part * 8, lanes) for g in g_refs], axis=0
            )
            back = dot(t_ref[...], (spec * weight).astype(BF))
            back = back.reshape(groups, chunks, depth, 8, lanes).astype(BF)
            for c in range(chunks):
                o_refs[c][:, :, i : i + 8, :] = back[:, c]

    out = jax.ShapeDtypeStruct((groups, depth, v, u), BF)
    at = lambda i, j: (0, i, j)
    whole = lambda i, j: (0, 0)
    return pl.pallas_call(
        body,
        grid=(v // rows, u // lanes),
        in_specs=[
            pl.BlockSpec((z, rows, lanes), at),
            *[pl.BlockSpec((part, rows, lanes), at)] * groups,
            pl.BlockSpec((k * 8, z * 8), whole),
            pl.BlockSpec((z * 8, k * 8), whole),
        ],
        out_specs=[pl.BlockSpec((groups, depth, rows, lanes), lambda i, j: (0, 0, i, j))] * chunks,
        out_shape=[out] * chunks,
        compiler_params=pltpu.CompilerParams(vmem_limit_bytes=60 * 2**20),
        cost_estimate=cost(32 * z * k * v * u, planes, *greens, planes),
        name="z_weight",
    )(planes, *greens, wide, tall)


def x_inverse(back, table, rank, step, pencils):
    groups, z, share, u = back.shape
    v = groups * share
    x = u // pencils

    def body(b_ref, t_ref, o_ref):
        rows = jnp.concatenate([b_ref[j, 0] for j in range(groups)], axis=0)
        o_ref[0] = dot_t(t_ref[...], rows).astype(BF)

    out = jax.ShapeDtypeStruct((z, x, v), BF)
    return on_rank(
        body,
        (z,),
        [
            pl.BlockSpec((groups, 1, share, u), lambda i, r: (0, i, 0, 0)),
            pl.BlockSpec((x, u), lambda i, r: (lax.rem(r[0] + step, pencils), 0)),
        ],
        pl.BlockSpec((1, x, v), lambda i, r: (i, 0, 0)),
        out,
        cost(2 * z * v * u * x, back, out),
    )(rank, back, table)


def y_inverse(returned, table, rank, scale, total, z_all, first):
    pencils = len(returned)
    z, x, v = returned[0].shape
    y = pencils * v

    def body(*refs):
        r_refs, t_refs, o_ref = refs[:pencils], refs[pencils : 2 * pencils], refs[-1]
        acc = dot(r_refs[0][0], t_refs[0][...])
        for p in range(1, pencils):
            acc += dot(r_refs[p][0], t_refs[p][...])
        o_ref[0] = acc * scale

    def rows_of(s):
        return lambda i, r: (lax.rem(r[0] + pencils - s, pencils), 0)

    specs = [pl.BlockSpec((1, x, v), lambda i, r: (i, 0, 0))] * pencils
    specs += [pl.BlockSpec((v, y), rows_of(s)) for s in range(pencils)]
    operands = [*returned, *[table] * pencils]
    aliases = {}
    if total is not None:
        aliases = {1 + len(operands): 0}
        specs.append(pl.BlockSpec(memory_space=pl.ANY))
        operands.append(total)
    return on_rank(
        body,
        (z,),
        specs,
        pl.BlockSpec((1, x, y), lambda i, r: (i + first, 0, 0)),
        jax.ShapeDtypeStruct((z_all, x, y), F32),
        cost(2 * z * x * y * y, *returned, *returned, *returned),
        input_output_aliases=aliases,
    )(rank, *operands)


def exchange(a, axis):
    return lax.all_to_all(a, axis, split_axis=0, concat_axis=0, tiled=True)


def local(density, green):
    z_slab, _, y_cells = density.shape
    k_block, y_local, x_cells = green.shape
    groups = lax.axis_size("gz")
    pencils = lax.axis_size("pa")
    z_cells = z_slab * groups
    z_freqs = k_block * groups
    share = y_local // groups
    g_rank = lax.axis_index("gz").astype(jnp.int32)
    p_rank = lax.axis_index("pa").astype(jnp.int32)
    g_me, p_me = g_rank.reshape(1), p_rank.reshape(1)
    greens = []
    for s in [*range(1, groups), 0]:
        piece = green_piece(green, g_me, s, groups)
        if s:
            piece = shift(piece, "gz", s)
        greens.append(piece)
    order = jnp.array([*range(1, groups), 0], dtype=jnp.int32)
    sources = (g_rank - order) % groups
    f_index = (sources[:, None] * k_block + jnp.arange(k_block, dtype=jnp.int32)).reshape(-1)
    cas_y = square_table(y_cells)
    cas_x = cas_y if x_cells == y_cells else square_table(x_cells)
    cas_m = cas_table(f_index, jnp.arange(z_cells, dtype=jnp.int32), z_freqs)
    moved = y_forward(density, cas_y, pencils)
    moved = exchange(moved, "pa")
    planes = x_forward(moved, cas_x, groups)
    planes = exchange(planes, "gz").reshape(z_cells, share, x_cells)
    chunks = math.gcd(z_slab, CHUNKS)
    scale = 1.0 / (x_cells * y_cells * z_freqs)
    potential = None
    for c, back in enumerate(z_weight(planes, greens, cas_m, chunks)):
        back = exchange(back, "gz")
        returned = [x_inverse(back, cas_x, p_me, s, pencils) for s in range(pencils)]
        returned = [shift(a, "pa", s) if s else a for s, a in enumerate(returned)]
        first = c * (z_slab // chunks)
        potential = y_inverse(returned, cas_y, p_me, scale, potential, z_slab, first)
    return potential


def solution(mesh):
    return jax.shard_map(
        local,
        mesh=mesh,
        in_specs=(P("gz", "pa", None), P("gz", "pa", None)),
        out_specs=P("gz", "pa", None),
        check_vma=False,
    )
```
